32 devices in a mesh: replica: 4 (over y, core), model: 8 (over z, x).
Axes of the slice: x: 2, y: 2, z: 4, core: 2. Of those that a mesh axis runs over, the one named last changes fastest.
Arguments:
- partial_query: float32 [4, 2048, 2048], P('replica', None, 'model'), may hold values from -4 to 4
- partial_key: float32 [4, 2048, 2048], P('replica', None, 'model'), may hold values from -4 to 4
- partial_value: float32 [4, 2048, 2048], P('replica', None, 'model'), may hold values from -4 to 4
- partial_mixed: float32 [4, 2048, 2048], P('replica', 'model'), may hold values from -4 to 4
- partial_norm: float32 [4, 2048], P('replica'), may hold values from -8 to 8
- partial_bias: float32 [4, 2048], P('replica'), may hold values from -8 to 8
- master_query: float32 [2048, 2048], P('replica', 'model'), may hold values from -0.1875 to 0.1875
- master_key: float32 [2048, 2048], P('replica', 'model'), may hold values from -0.1875 to 0.1875
- master_value: float32 [2048, 2048], P('replica', 'model'), may hold values from -0.1875 to 0.1875
- master_mixed: float32 [2048, 2048], P('model', 'replica'), may hold values from -0.1875 to 0.1875
- master_norm: float32 [2048], P('replica'), may hold values from 0.25 to 1.75
- master_bias: float32 [2048], P('replica'), may hold values from -3 to 3
- memory_query: float32 [2048, 2048], P('replica', 'model'), may hold values from 9.765625e-05 to 0.0009765625
- memory_key: float32 [2048, 2048], P('replica', 'model'), may hold values from 9.765625e-05 to 0.0009765625
- memory_value: float32 [2048, 2048], P('replica', 'model'), may hold values from 9.765625e-05 to 0.0009765625
- memory_mixed: float32 [2048, 2048], P('model', 'replica'), may hold values from 9.765625e-05 to 0.0009765625
- memory_norm: float32 [2048], P('replica'), may hold values from 0.05 to 0.8
- memory_bias: float32 [2048], P('replica'), may hold values from 0.05 to 0.8
Outputs:
- compute_query: bfloat16 [2048, 2048], P(None, 'model')
- compute_key: bfloat16 [2048, 2048], P(None, 'model')
- compute_value: bfloat16 [2048, 2048], P(None, 'model')
- compute_mixed: bfloat16 [2048, 2048], P('model')
- compute_norm: bfloat16 [2048], replicated
- compute_bias: bfloat16 [2048], replicated
- stepped_query: float32 [2048, 2048], P('replica', 'model')
- stepped_key: float32 [2048, 2048], P('replica', 'model')
- stepped_value: float32 [2048, 2048], P('replica', 'model')
- stepped_mixed: float32 [2048, 2048], P('model', 'replica')
- stepped_norm: float32 [2048], P('replica')
- stepped_bias: float32 [2048], P('replica')
- state_new_query: float32 [2048, 2048], P('replica', 'model')
- state_new_key: float32 [2048, 2048], P('replica', 'model')
- state_new_value: float32 [2048, 2048], P('replica', 'model')
- state_new_mixed: float32 [2048, 2048], P('model', 'replica')
- state_new_norm: float32 [2048], P('replica')
- state_new_bias: float32 [2048], P('replica')
The draws below stay inside these ranges and needn't reach their ends.
All inputs are finite; a program needn't handle non-finite values.
Results may differ from the reference program's by a relative error of at most 0.0004.
Values may be sent and summed in bfloat16 or wider, within the bound.
No kernel may reach another device: no remote copies, remote signals or barrier semaphores. Data moves between devices by JAX's collectives and lax.ppermute only.
A program may use at most 64 MiB of HBM per device.

```python
import jax
import jax.numpy as jnp
from jax import lax

WIDTH = 2048
ATTN = 2048
REPLICAS = 4


def with_spikes(drawn, stream_key, source, target, shards_of, factor):
    def block_of(axis_at):
        return (jnp.arange(drawn.shape[axis_at]) // (drawn.shape[axis_at] // shards_of)).reshape((-1,) + (1,) * (drawn.ndim - 1 - axis_at))

    first = jax.random.permutation(stream_key, shards_of)[block_of(target)]
    second = (block_of(target) + shards_of // 2) % shards_of
    return jnp.where((block_of(source) == first) | (block_of(source) == second), factor * drawn, drawn)


def block_scale(key, extent, split, smallest, high):
    gain, own = 1.0, jax.random.fold_in(key, 6)
    for dim, parts in split:
        draws = jnp.exp(jax.random.uniform(jax.random.fold_in(own, dim), (parts,), jnp.float32, smallest / len(split), high / len(split)))
        gain = gain * jnp.repeat(draws, extent[dim] // parts).reshape([-1 if axis == dim else 1 for axis in range(len(extent))])
    return gain


def noise(rng, shape, scale, reach, split=(), dtype=jnp.bfloat16):
    values = jax.random.normal(rng, shape, jnp.float32) * scale
    if len(split) > 0:
        values = block_scale(rng, shape, split, -0.22, 0.18) * values
    return jnp.clip(values, min=-reach, max=reach).astype(dtype)


def gaussian_with(own_key, dims, width, bound, pieces, heavy, held_as=jnp.bfloat16):
    array = width * jax.random.normal(own_key, dims, jnp.float32)
    if pieces:
        array = array * block_scale(own_key, dims, pieces, -0.22, 0.18)
    return jnp.clip(with_spikes(array, jax.random.fold_in(own_key, 3), *heavy), -bound, bound).astype(held_as)


def setup_inputs(seed: int = 0) -> dict:
    keys = jax.random.split(jax.random.key(seed), 19)
    return {
        "partial_query": gaussian_with(keys[0], (REPLICAS, WIDTH, ATTN), 0.5, 4.0, ((0, 4), (2, 8)), (0, 1, 4, 2.0), jnp.float32),
        "partial_key": gaussian_with(keys[1], (REPLICAS, WIDTH, ATTN), 0.5, 4.0, ((0, 4), (2, 8)), (0, 1, 4, 2.0), jnp.float32),
        "partial_value": gaussian_with(keys[2], (REPLICAS, WIDTH, ATTN), 0.5, 4.0, ((0, 4), (2, 8)), (0, 1, 4, 2.0), jnp.float32),
        "partial_mixed": gaussian_with(keys[3], (REPLICAS, ATTN, WIDTH), 0.5, 4.0, ((0, 4), (1, 8)), (0, 2, 4, 2.0), jnp.float32),
        "partial_norm": gaussian_with(keys[4], (REPLICAS, WIDTH), 1.0, 8.0, ((0, 4),), (0, 1, 4, 2.0), jnp.float32),
        "partial_bias": gaussian_with(keys[5], (REPLICAS, WIDTH), 1.0, 8.0, ((0, 4),), (0, 1, 4, 2.0), jnp.float32),
        "master_query": gaussian_with(keys[6], (WIDTH, ATTN), WIDTH ** -0.5, 0.1875, ((0, 4), (1, 8)), (1, 0, 8, 2.0), jnp.float32),
        "master_key": gaussian_with(keys[7], (WIDTH, ATTN), WIDTH ** -0.5, 0.1875, ((0, 4), (1, 8)), (1, 0, 8, 2.0), jnp.float32),
        "master_value": gaussian_with(keys[8], (WIDTH, ATTN), WIDTH ** -0.5, 0.1875, ((0, 4), (1, 8)), (1, 0, 8, 2.0), jnp.float32),
        "master_mixed": gaussian_with(keys[9], (ATTN, WIDTH), ATTN ** -0.5, 0.1875, ((0, 8), (1, 4)), (0, 1, 8, 2.0), jnp.float32),
        "master_norm": jnp.clip(1.0 + 0.15 * jax.random.normal(keys[10], (WIDTH,), jnp.float32), 0.25, 1.75),
        "master_bias": noise(keys[11], (WIDTH,), 0.5, 3.0, ((0, 4),), jnp.float32),
        "memory_query": jnp.clip(9.765625145519152e-05 + 0.0008789062 * jax.random.uniform(keys[12], (WIDTH, ATTN), jnp.float32) ** block_scale(keys[12], (WIDTH, ATTN), ((0, 4), (1, 8)), -0.2, 0.2), 9.765625145519152e-05, 0.0009765625),
        "memory_key": jnp.clip(9.765625145519152e-05 + 0.0008789062 * jax.random.uniform(keys[13], (WIDTH, ATTN), jnp.float32) ** block_scale(keys[13], (WIDTH, ATTN), ((0, 4), (1, 8)), -0.2, 0.2), 9.765625145519152e-05, 0.0009765625),
        "memory_value": jnp.clip(9.765625145519152e-05 + 0.0008789062 * jax.random.uniform(keys[14], (WIDTH, ATTN), jnp.float32) ** block_scale(keys[14], (WIDTH, ATTN), ((0, 4), (1, 8)), -0.2, 0.2), 9.765625145519152e-05, 0.0009765625),
        "memory_mixed": jnp.clip(9.765625145519152e-05 + 0.0008789062 * jax.random.uniform(keys[15], (ATTN, WIDTH), jnp.float32) ** block_scale(keys[15], (ATTN, WIDTH), ((0, 8), (1, 4)), -0.2, 0.2), 9.765625145519152e-05, 0.0009765625),
        "memory_norm": jnp.clip(0.05 + 0.75 * jax.random.uniform(keys[16], (WIDTH,), jnp.float32) ** block_scale(keys[16], (WIDTH,), ((0, 4),), -0.2, 0.2), 0.05, 0.8),
        "memory_bias": jnp.clip(0.05 + 0.75 * jax.random.uniform(keys[17], (WIDTH,), jnp.float32) ** block_scale(keys[17], (WIDTH,), ((0, 4),), -0.2, 0.2), 0.05, 0.8),
    }


learn_rate = 0.015
hold_rate = 0.8

def reference(partial_query, partial_key, partial_value, partial_mixed, partial_norm, partial_bias, master_query, master_key, master_value, master_mixed, master_norm, master_bias, memory_query, memory_key, memory_value, memory_mixed, memory_norm, memory_bias):
    mean_query = lax.optimization_barrier(jnp.sum(partial_query.astype(jnp.float32), axis=0)) * REPLICAS ** (-0.5)
    mean_key = lax.optimization_barrier(jnp.sum(partial_key.astype(jnp.float32), axis=0)) * REPLICAS ** (-0.5)
    mean_value = lax.optimization_barrier(jnp.sum(partial_value.astype(jnp.float32), axis=0)) * REPLICAS ** (-0.5)
    mean_mixed = lax.optimization_barrier(jnp.sum(partial_mixed.astype(jnp.float32), axis=0)) * REPLICAS ** (-0.5)
    mean_norm = lax.optimization_barrier(jnp.sum(partial_norm.astype(jnp.float32), axis=0)) * REPLICAS ** (-0.5)
    mean_bias = lax.optimization_barrier(jnp.sum(partial_bias.astype(jnp.float32), axis=0)) * REPLICAS ** (-0.5)
    ratio_query = jnp.sqrt(lax.optimization_barrier(jnp.sum(master_query * master_query, axis=1, keepdims=True))) * lax.rsqrt(lax.optimization_barrier(jnp.sum(mean_query * mean_query, axis=1, keepdims=True)) + 1e-06)
    mean_query = mean_query * ratio_query
    ratio_key = jnp.sqrt(lax.optimization_barrier(jnp.sum(master_key * master_key, axis=1, keepdims=True))) * lax.rsqrt(lax.optimization_barrier(jnp.sum(mean_key * mean_key, axis=1, keepdims=True)) + 1e-06)
    mean_key = mean_key * ratio_key
    ratio_value = jnp.sqrt(lax.optimization_barrier(jnp.sum(master_value * master_value, axis=1, keepdims=True))) * lax.rsqrt(lax.optimization_barrier(jnp.sum(mean_value * mean_value, axis=1, keepdims=True)) + 1e-06)
    mean_value = mean_value * ratio_value
    ratio_mixed = jnp.sqrt(lax.optimization_barrier(jnp.sum(master_mixed * master_mixed, axis=0, keepdims=True))) * lax.rsqrt(lax.optimization_barrier(jnp.sum(mean_mixed * mean_mixed, axis=0, keepdims=True)) + 1e-06)
    mean_mixed = mean_mixed * ratio_mixed
    state_new_query = hold_rate * memory_query + (1.0 - hold_rate) * mean_query * mean_query
    stepped_query = master_query - learn_rate * mean_query * lax.rsqrt(state_new_query + 1e-06)
    state_new_key = hold_rate * memory_key + (1.0 - hold_rate) * mean_key * mean_key
    stepped_key = master_key - learn_rate * mean_key * lax.rsqrt(state_new_key + 1e-06)
    state_new_value = hold_rate * memory_value + (1.0 - hold_rate) * mean_value * mean_value
    stepped_value = master_value - learn_rate * mean_value * lax.rsqrt(state_new_value + 1e-06)
    state_new_mixed = hold_rate * memory_mixed + (1.0 - hold_rate) * mean_mixed * mean_mixed
    stepped_mixed = master_mixed - learn_rate * mean_mixed * lax.rsqrt(state_new_mixed + 1e-06)
    state_new_norm = hold_rate * memory_norm + (1.0 - hold_rate) * mean_norm * mean_norm
    stepped_norm = master_norm - learn_rate * mean_norm * lax.rsqrt(state_new_norm + 1e-06)
    state_new_bias = hold_rate * memory_bias + (1.0 - hold_rate) * mean_bias * mean_bias
    stepped_bias = master_bias - learn_rate * mean_bias * lax.rsqrt(state_new_bias + 1e-06)
    compute_query = stepped_query.astype(jnp.bfloat16)
    compute_key = stepped_key.astype(jnp.bfloat16)
    compute_value = stepped_value.astype(jnp.bfloat16)
    compute_mixed = stepped_mixed.astype(jnp.bfloat16)
    compute_norm = stepped_norm.astype(jnp.bfloat16)
    compute_bias = stepped_bias.astype(jnp.bfloat16)
    return (compute_query, compute_key, compute_value, compute_mixed, compute_norm, compute_bias, stepped_query, stepped_key, stepped_value, stepped_mixed, stepped_norm, stepped_bias, state_new_query, state_new_key, state_new_value, state_new_mixed, state_new_norm, state_new_bias)
```

```python
import jax
import jax.numpy as jnp
from jax import lax
from jax.sharding import PartitionSpec as P


learn_rate = 0.015
hold_rate = 0.8

half_bound = 8.0
wire_scale = 60000.0 / half_bound**1.5


names = ("query", "key", "value", "mixed")


def block_of(whole, index, count, axis):
    if axis == 0:
        split = whole.reshape(count, whole.shape[0] // count, whole.shape[1])
        return lax.dynamic_index_in_dim(split, index, axis=0, keepdims=False)
    size = whole.shape[1] // count
    return lax.dynamic_slice_in_dim(whole, index * size, size, axis=1)


def put_block(whole, block, index, count, axis):
    if axis == 0:
        split = whole.reshape(count, whole.shape[0] // count, whole.shape[1])
        return lax.dynamic_update_index_in_dim(split, block[None], index, axis=0).reshape(whole.shape)
    return lax.dynamic_update_slice_in_dim(whole, block, index * block.shape[1], axis=1)


def shards(*args):
    partial = dict(zip(names, (a[0] for a in args[0:4])))
    partial_vectors = jnp.stack([args[4][0], args[5][0]])
    master = dict(zip(names, args[6:10]))
    master_vectors = jnp.stack(args[10:12])
    memory = dict(zip(names, args[12:16]))
    memory_vectors = jnp.stack(args[16:18])
    axis_of = {"query": 0, "key": 0, "value": 0, "mixed": 1}

    count = lax.axis_size("replica")
    width = 2 if count % 2 == 0 else 1
    chips = count // width
    place = lax.axis_index("replica")
    chip, core = place // width, place % width
    models = lax.axis_size("model")
    mean_rate = count ** (-0.5)

    def to_pair(value):
        return lax.ppermute(value, "replica", [(i, i ^ 1) for i in range(count)])

    def to_chip(value, step):
        pairs = [
            (i, (i // width + step) % chips * width + i % width) for i in range(count)
        ]
        return lax.ppermute(value, "replica", pairs)

    def after(value, *others):
        return lax.optimization_barrier((value, *others))[0]

    def encode(value):
        size = jnp.abs(value)
        root = size * lax.rsqrt(jnp.maximum(size, 1e-30))
        return (value * root * wire_scale).astype(jnp.float16)

    def decode(code):
        code = code.astype(jnp.float32)
        size = jnp.exp(jnp.log(jnp.abs(code) * (1.0 / wire_scale)) * (2.0 / 3.0))
        return jnp.where(code < 0, -size, size)

    def other(step):
        return (chip + step) % chips * width + core

    def paired(n, step):
        own = block_of(partial[n], other(step), count, axis_of[n])
        if width == 1:
            return own
        theirs = block_of(partial[n], other(step) ^ 1, count, axis_of[n])
        return own + to_pair(theirs)

    own_vectors = jnp.concatenate([master_vectors, memory_vectors])
    vector_sum, vector_all = partial_vectors, jnp.zeros((count,) + own_vectors.shape, jnp.float32)
    vector_all = lax.dynamic_update_index_in_dim(vector_all, own_vectors[None], place, axis=0)
    packed = jnp.concatenate([partial_vectors.reshape(-1), own_vectors.reshape(-1)])
    split = partial_vectors.size
    vector_got = [to_chip(packed, step) for step in range(1, chips)]

    arrived = {}
    for n in names:
        arrived[n] = []
        for step in range(1, chips):
            arrived[n].append(to_chip(encode(paired(n, step)), step))

    for step, got in enumerate(vector_got, 1):
        got = after(got, *arrived["query"])
        vector_sum = vector_sum + got[:split].reshape(partial_vectors.shape)
        vector_all = lax.dynamic_update_index_in_dim(
            vector_all,
            got[split:].reshape(own_vectors.shape)[None],
            (chip - step) % chips * width + core,
            axis=0,
        )

    mean, outs = {}, {}

    def reduce(n, *others):
        total = paired(n, 0)
        for piece in arrived[n]:
            total = total + decode(after(piece, *others))
        mean[n] = total * mean_rate
        return jnp.sum(mean[n] * mean[n], axis=1 - axis_of[n])

    def own_size(n):
        held = after(master[n], *arrived["query"])
        return jnp.sum(held * held, axis=1 - axis_of[n])

    def finish(n, own, slope):
        ratio = jnp.sqrt(own) * lax.rsqrt(slope + 1e-06)
        scaled = mean[n] * jnp.expand_dims(ratio, 1 - axis_of[n])
        state_new = hold_rate * memory[n] + (1.0 - hold_rate) * scaled * scaled
        stepped = master[n] - learn_rate * scaled * lax.rsqrt(state_new + 1e-06)
        compute = stepped.astype(jnp.bfloat16)
        pieces = [(compute, place)]
        for step in range(1, chips):
            pieces.append((to_chip(compute, step), (chip - step) % chips * width + core))
        outs[n] = (pieces, stepped, state_new)
        return compute

    def gather(n, *others):
        pieces, stepped, state_new = outs[n]
        whole = jnp.zeros(partial[n].shape, jnp.bfloat16)
        for piece, index in pieces:
            whole = put_block(whole, piece, index, count, axis_of[n])
            if width == 2:
                whole = put_block(whole, to_pair(piece), index ^ 1, count, axis_of[n])
        outs[n] = (whole, stepped, state_new)

    def stages(value):
        if models & (models - 1):
            return [lax.psum(value, "model")]
        found, bit = [], 1
        while bit < models:
            got = lax.ppermute(value, "model", [(i, i ^ bit) for i in range(models)])
            value = value + got
            found.append(value)
            bit *= 2
        return found

    slope_q = reduce("query")
    slope_k = reduce("key")
    first = stages(jnp.stack([own_size("query"), own_size("key"), slope_q, slope_k]))
    slope_v = reduce("value", first[0])
    slope_m = reduce("mixed", first[-1])
    second = stages(jnp.stack([own_size("value"), own_size("mixed"), slope_v, slope_m]))
    total = first[-1]
    finish("query", total[0], total[2])
    finish("key", total[1], total[3])
    total = second[-1]
    finish("value", total[0], total[2])
    finish("mixed", total[1], total[3])
    for n in names:
        gather(n)

    if width == 2:
        vector_sum = vector_sum + to_pair(vector_sum)
        theirs = to_pair(vector_all)
        held = (jnp.arange(count) % width == core)[:, None, None]
        vector_all = jnp.where(held, vector_all, theirs)
    vector_mean = vector_sum * mean_rate
    vector_all = vector_all.transpose(1, 0, 2).reshape(4, -1)
    state_whole = hold_rate * vector_all[2:] + (1.0 - hold_rate) * vector_mean * vector_mean
    stepped_whole = vector_all[:2] - learn_rate * vector_mean * lax.rsqrt(state_whole + 1e-06)
    compute_vectors = stepped_whole.astype(jnp.bfloat16)
    own = args[10].shape[0]
    stepped_own = lax.dynamic_slice_in_dim(stepped_whole, place * own, own, axis=1)
    state_own = lax.dynamic_slice_in_dim(state_whole, place * own, own, axis=1)
    return (
        *(outs[n][0] for n in names),
        compute_vectors[0],
        compute_vectors[1],
        *(outs[n][1] for n in names),
        stepped_own[0],
        stepped_own[1],
        *(outs[n][2] for n in names),
        state_own[0],
        state_own[1],
    )


def solution(mesh):
    rows, columns = P("replica", "model"), P("model", "replica")
    in_specs = (
        *(P("replica", None, "model"),) * 3,
        P("replica", "model", None),
        *(P("replica", None),) * 2,
        *((rows,) * 3 + (columns,) + (P("replica"),) * 2) * 2,
    )
    out_specs = (
        *(P(None, "model"),) * 3,
        P("model", None),
        P(),
        P(),
        *((rows,) * 3 + (columns,) + (P("replica"),) * 2) * 2,
    )

    return jax.shard_map(shards, mesh=mesh, in_specs=in_specs, out_specs=out_specs, check_vma=False)
```

```python
import jax
import jax.numpy as jnp
from jax import lax
from jax.sharding import PartitionSpec as P


learn_rate = 0.015
hold_rate = 0.8

code_scale = 200.0
code_power = 12


names = ("query", "key", "value", "mixed")


def block_of(whole, index, count, axis):
    if axis == 0:
        split = whole.reshape(count, whole.shape[0] // count, whole.shape[1])
        return lax.dynamic_index_in_dim(split, index, axis=0, keepdims=False)
    size = whole.shape[1] // count
    return lax.dynamic_slice_in_dim(whole, index * size, size, axis=1)


def put_block(whole, block, index, count, axis):
    if axis == 0:
        split = whole.reshape(count, whole.shape[0] // count, whole.shape[1])
        return lax.dynamic_update_index_in_dim(split, block[None], index, axis=0).reshape(whole.shape)
    return lax.dynamic_update_slice_in_dim(whole, block, index * block.shape[1], axis=1)


def shards(*args):
    partial = dict(zip(names, (a[0] for a in args[0:4])))
    partial_vectors = jnp.stack([args[4][0], args[5][0]])
    master = dict(zip(names, args[6:10]))
    master_vectors = jnp.stack(args[10:12])
    memory = dict(zip(names, args[12:16]))
    memory_vectors = jnp.stack(args[16:18])
    axis_of = {"query": 0, "key": 0, "value": 0, "mixed": 1}

    count = lax.axis_size("replica")
    width = 2 if count % 2 == 0 else 1
    chips = count // width
    place = lax.axis_index("replica")
    chip, core = place // width, place % width
    models = lax.axis_size("model")
    mean_rate = count ** (-0.5)

    def to_pair(value):
        return lax.ppermute(value, "replica", [(i, i ^ 1) for i in range(count)])

    def to_chip(value, step):
        pairs = [
            (i, (i // width + step) % chips * width + i % width) for i in range(count)
        ]
        return lax.ppermute(value, "replica", pairs)

    def after(value, *others):
        return lax.optimization_barrier((value, *others))[0]

    def encode(value):
        value = value * code_scale
        cube = value * value * value
        size = (cube * cube) * (cube * cube)
        return jnp.where(value < 0, -size, size).astype(jnp.bfloat16)

    def decode(code):
        code = code.astype(jnp.float32)
        size = jnp.exp(jnp.log(jnp.abs(code)) * (1.0 / code_power)) * (1.0 / code_scale)
        return jnp.where(code < 0, -size, size)

    def other(step):
        return (chip + step) % chips * width + core

    early = "query"

    def paired(n, step):
        own = block_of(partial[n], other(step), count, axis_of[n])
        if width == 1:
            return own
        if n == early and step == 1:
            theirs = block_of(partial[n], other(step) ^ 1, count, axis_of[n])
            return own + to_pair(theirs)
        return own + block_of(crossed[n], other(step), count, axis_of[n])

    crossed = {n: to_pair(partial[n]) for n in names} if width == 2 else {}

    own_vectors = jnp.concatenate([master_vectors, memory_vectors])
    vector_sum, vector_all = partial_vectors, jnp.zeros((count,) + own_vectors.shape, jnp.float32)
    vector_all = lax.dynamic_update_index_in_dim(vector_all, own_vectors[None], place, axis=0)
    packed = jnp.concatenate([partial_vectors.reshape(-1), own_vectors.reshape(-1)])
    split = partial_vectors.size
    vector_got = [to_chip(packed, step) for step in range(1, chips)]

    arrived = {}
    for n in names:
        arrived[n] = []
        for step in range(1, chips):
            code = encode(paired(n, step))
            arrived[n].append(to_chip(code, step))

    for step, got in enumerate(vector_got, 1):
        got = after(got, *arrived["query"])
        vector_sum = vector_sum + got[:split].reshape(partial_vectors.shape)
        vector_all = lax.dynamic_update_index_in_dim(
            vector_all,
            got[split:].reshape(own_vectors.shape)[None],
            (chip - step) % chips * width + core,
            axis=0,
        )

    mean, outs = {}, {}

    def reduce_in(n, *others):
        total = paired(n, 0)
        for piece in arrived[n]:
            total = total + decode(after(piece, *others))
        mean[n] = total * mean_rate
        return jnp.sum(mean[n] * mean[n], axis=1 - axis_of[n])

    def own_size(n):
        held = after(master[n], *arrived["query"])
        return jnp.sum(held * held, axis=1 - axis_of[n])

    def finish(n, own, slope):
        ratio = jnp.sqrt(own) * lax.rsqrt(slope + 1e-06)
        scaled = mean[n] * jnp.expand_dims(ratio, 1 - axis_of[n])
        state_new = hold_rate * memory[n] + (1.0 - hold_rate) * scaled * scaled
        stepped = master[n] - learn_rate * scaled * lax.rsqrt(state_new + 1e-06)
        compute = stepped.astype(jnp.bfloat16)
        pieces = [(compute, place)]
        for step in range(1, chips):
            pieces.append((to_chip(compute, step), (chip - step) % chips * width + core))
        outs[n] = (pieces, stepped, state_new)
        return compute

    def gather(n, *others):
        pieces, stepped, state_new = outs[n]
        whole = jnp.zeros(partial[n].shape, jnp.bfloat16)
        for piece, index in pieces:
            whole = put_block(whole, piece, index, count, axis_of[n])
            if width == 2:
                whole = put_block(whole, to_pair(piece), index ^ 1, count, axis_of[n])
        outs[n] = (whole, stepped, state_new)

    def stages(value):
        if models & (models - 1):
            return [lax.psum(value, "model")]
        found, bit = [], 1
        while bit < models:
            got = lax.ppermute(value, "model", [(i, i ^ bit) for i in range(models)])
            value = value + got
            found.append(value)
            bit *= 2
        return found

    slope_q = reduce_in("query")
    slope_k = reduce_in("key")
    first = stages(jnp.stack([own_size("query"), own_size("key"), slope_q, slope_k]))
    slope_v = reduce_in("value", first[0])
    slope_m = reduce_in("mixed", first[-1])
    second = stages(jnp.stack([own_size("value"), own_size("mixed"), slope_v, slope_m]))
    total = first[-1]
    finish("query", total[0], total[2])
    finish("key", total[1], total[3])
    total = second[-1]
    finish("value", total[0], total[2])
    finish("mixed", total[1], total[3])
    for n in names:
        gather(n)

    if width == 2:
        vector_sum = vector_sum + to_pair(vector_sum)
        theirs = to_pair(vector_all)
        held = (jnp.arange(count) % width == core)[:, None, None]
        vector_all = jnp.where(held, vector_all, theirs)
    vector_mean = vector_sum * mean_rate
    vector_all = vector_all.transpose(1, 0, 2).reshape(4, -1)
    state_whole = hold_rate * vector_all[2:] + (1.0 - hold_rate) * vector_mean * vector_mean
    stepped_whole = vector_all[:2] - learn_rate * vector_mean * lax.rsqrt(state_whole + 1e-06)
    compute_vectors = stepped_whole.astype(jnp.bfloat16)
    own = args[10].shape[0]
    stepped_own = lax.dynamic_slice_in_dim(stepped_whole, place * own, own, axis=1)
    state_own = lax.dynamic_slice_in_dim(state_whole, place * own, own, axis=1)
    return (
        *(outs[n][0] for n in names),
        compute_vectors[0],
        compute_vectors[1],
        *(outs[n][1] for n in names),
        stepped_own[0],
        stepped_own[1],
        *(outs[n][2] for n in names),
        state_own[0],
        state_own[1],
    )


def solution(mesh):
    rows, columns = P("replica", "model"), P("model", "replica")
    in_specs = (
        *(P("replica", None, "model"),) * 3,
        P("replica", "model", None),
        *(P("replica", None),) * 2,
        *((rows,) * 3 + (columns,) + (P("replica"),) * 2) * 2,
    )
    out_specs = (
        *(P(None, "model"),) * 3,
        P("model", None),
        P(),
        P(),
        *((rows,) * 3 + (columns,) + (P("replica"),) * 2) * 2,
    )

    return jax.shard_map(shards, mesh=mesh, in_specs=in_specs, out_specs=out_specs, check_vma=False)
```

```python
import jax
import jax.numpy as jnp
from jax import lax
from jax.sharding import PartitionSpec as P


learn_rate = 0.015
hold_rate = 0.8

code_scale = 200.0
code_power = 12


names = ("query", "key", "value", "mixed")


def block_of(whole, index, count, axis):
    if axis == 0:
        split = whole.reshape(count, whole.shape[0] // count, whole.shape[1])
        return lax.dynamic_index_in_dim(split, index, axis=0, keepdims=False)
    size = whole.shape[1] // count
    return lax.dynamic_slice_in_dim(whole, index * size, size, axis=1)


def put_block(whole, block, index, count, axis):
    if axis == 0:
        split = whole.reshape(count, whole.shape[0] // count, whole.shape[1])
        return lax.dynamic_update_index_in_dim(split, block[None], index, axis=0).reshape(whole.shape)
    return lax.dynamic_update_slice_in_dim(whole, block, index * block.shape[1], axis=1)


def shards(*args):
    partial = dict(zip(names, (a[0] for a in args[0:4])))
    partial_vectors = jnp.stack([args[4][0], args[5][0]])
    master = dict(zip(names, args[6:10]))
    master_vectors = jnp.stack(args[10:12])
    memory = dict(zip(names, args[12:16]))
    memory_vectors = jnp.stack(args[16:18])
    axis_of = {"query": 0, "key": 0, "value": 0, "mixed": 1}

    count = lax.axis_size("replica")
    width = 2 if count % 2 == 0 else 1
    chips = count // width
    place = lax.axis_index("replica")
    chip, core = place // width, place % width
    models = lax.axis_size("model")
    mean_rate = count ** (-0.5)

    def to_pair(value):
        return lax.ppermute(value, "replica", [(i, i ^ 1) for i in range(count)])

    def to_chip(value, step):
        pairs = [
            (i, (i // width + step) % chips * width + i % width) for i in range(count)
        ]
        return lax.ppermute(value, "replica", pairs)

    def after(value, *others):
        return lax.optimization_barrier((value, *others))[0]

    def encode(value):
        value = value * code_scale
        cube = value * value * value
        size = (cube * cube) * (cube * cube)
        return jnp.where(value < 0, -size, size).astype(jnp.bfloat16)

    def decode(code):
        code = code.astype(jnp.float32)
        size = jnp.exp(jnp.log(jnp.abs(code)) * (1.0 / code_power)) * (1.0 / code_scale)
        return jnp.where(code < 0, -size, size)

    def other(step):
        return (chip + step) % chips * width + core

    early = "query"

    def paired(n, step):
        own = block_of(partial[n], other(step), count, axis_of[n])
        if width == 1:
            return own
        if n == early and step == 1:
            theirs = block_of(partial[n], other(step) ^ 1, count, axis_of[n])
            return own + to_pair(theirs)
        return own + block_of(crossed[n], other(step), count, axis_of[n])

    crossed = {n: to_pair(partial[n]) for n in names} if width == 2 else {}

    own_vectors = jnp.concatenate([master_vectors, memory_vectors])
    vector_sum, vector_all = partial_vectors, jnp.zeros((count,) + own_vectors.shape, jnp.float32)
    vector_all = lax.dynamic_update_index_in_dim(vector_all, own_vectors[None], place, axis=0)
    packed = jnp.concatenate([partial_vectors.reshape(-1), own_vectors.reshape(-1)])
    split = partial_vectors.size
    vector_got = [to_chip(packed, step) for step in range(1, chips)]

    arrived = {}
    for n in names:
        arrived[n] = []
        for step in range(1, chips):
            code = encode(paired(n, step))
            arrived[n].append(to_chip(code, step))

    for step, got in enumerate(vector_got, 1):
        got = after(got, *arrived["query"])
        vector_sum = vector_sum + got[:split].reshape(partial_vectors.shape)
        vector_all = lax.dynamic_update_index_in_dim(
            vector_all,
            got[split:].reshape(own_vectors.shape)[None],
            (chip - step) % chips * width + core,
            axis=0,
        )

    mean, outs = {}, {}

    def reduce_in(n, *others):
        total = paired(n, 0)
        for piece in arrived[n]:
            total = total + decode(after(piece, *others))
        mean[n] = total * mean_rate
        return jnp.sum(mean[n] * mean[n], axis=1 - axis_of[n])

    def own_size(n):
        held = after(master[n], *arrived["query"])
        return jnp.sum(held * held, axis=1 - axis_of[n])

    def finish(n, own, slope):
        ratio = jnp.sqrt(own) * lax.rsqrt(slope + 1e-06)
        scaled = mean[n] * jnp.expand_dims(ratio, 1 - axis_of[n])
        state_new = hold_rate * memory[n] + (1.0 - hold_rate) * scaled * scaled
        stepped = master[n] - learn_rate * scaled * lax.rsqrt(state_new + 1e-06)
        compute = stepped.astype(jnp.bfloat16)
        pieces = [(compute, place)]
        for step in range(1, chips):
            pieces.append((to_chip(compute, step), (chip - step) % chips * width + core))
        outs[n] = (pieces, stepped, state_new)
        return compute

    def gather(n, *others):
        pieces, stepped, state_new = outs[n]
        whole = jnp.zeros(partial[n].shape, jnp.bfloat16)
        for piece, index in pieces:
            whole = put_block(whole, piece, index, count, axis_of[n])
            if width == 2:
                whole = put_block(whole, to_pair(piece), index ^ 1, count, axis_of[n])
        outs[n] = (whole, stepped, state_new)

    def stages(value):
        if models & (models - 1):
            return [lax.psum(value, "model")]
        bits = [1 << i for i in range(models.bit_length() - 1)]
        groups = [bits[:1]] + [bits[i : i + 2] for i in range(1, len(bits), 2)]
        found = []
        for group in groups:
            flips = [*group[::-1], sum(group)] if len(group) > 1 else group
            total = value
            for flip in flips:
                pairs = [(i, i ^ flip) for i in range(models)]
                total = total + lax.ppermute(value, "model", pairs)
            value = total
            found.append(value)
        return found

    slope_q = reduce_in("query")
    slope_k = reduce_in("key")
    first = stages(jnp.stack([own_size("query"), own_size("key"), slope_q, slope_k]))
    slope_v = reduce_in("value", first[0])
    slope_m = reduce_in("mixed", first[0])
    second = stages(jnp.stack([own_size("value"), own_size("mixed"), slope_v, slope_m]))
    total = first[-1]
    finish("query", total[0], total[2])
    finish("key", total[1], total[3])
    total = second[-1]
    finish("value", total[0], total[2])
    finish("mixed", total[1], total[3])
    for n in names:
        gather(n)

    if width == 2:
        vector_sum = vector_sum + to_pair(vector_sum)
        theirs = to_pair(vector_all)
        held = (jnp.arange(count) % width == core)[:, None, None]
        vector_all = jnp.where(held, vector_all, theirs)
    vector_mean = vector_sum * mean_rate
    vector_all = vector_all.transpose(1, 0, 2).reshape(4, -1)
    state_whole = hold_rate * vector_all[2:] + (1.0 - hold_rate) * vector_mean * vector_mean
    stepped_whole = vector_all[:2] - learn_rate * vector_mean * lax.rsqrt(state_whole + 1e-06)
    compute_vectors = stepped_whole.astype(jnp.bfloat16)
    own = args[10].shape[0]
    stepped_own = lax.dynamic_slice_in_dim(stepped_whole, place * own, own, axis=1)
    state_own = lax.dynamic_slice_in_dim(state_whole, place * own, own, axis=1)
    return (
        *(outs[n][0] for n in names),
        compute_vectors[0],
        compute_vectors[1],
        *(outs[n][1] for n in names),
        stepped_own[0],
        stepped_own[1],
        *(outs[n][2] for n in names),
        state_own[0],
        state_own[1],
    )


def solution(mesh):
    rows, columns = P("replica", "model"), P("model", "replica")
    in_specs = (
        *(P("replica", None, "model"),) * 3,
        P("replica", "model", None),
        *(P("replica", None),) * 2,
        *((rows,) * 3 + (columns,) + (P("replica"),) * 2) * 2,
    )
    out_specs = (
        *(P(None, "model"),) * 3,
        P("model", None),
        P(),
        P(),
        *((rows,) * 3 + (columns,) + (P("replica"),) * 2) * 2,
    )

    return jax.shard_map(shards, mesh=mesh, in_specs=in_specs, out_specs=out_specs, check_vma=False)
```
